32 devices in a mesh: grp: 2 (over y), seq: 4 (over z), head: 4 (over x, core).
Axes of the slice: x: 2, y: 2, z: 4, core: 2. Of those that a mesh axis runs over, the one named last changes fastest.
Arguments:
- draft_features: bfloat16 [2048, 8192], P(('grp', 'seq'), 'head'), parts along dimension 0, may hold values from -6 to 6
- w_key: bfloat16 [8192, 1024], P(None, 'head'), may hold values from -0.0625 to 0.0625
- w_value: bfloat16 [8192, 1024], P(None, 'head'), may hold values from -0.0625 to 0.0625
- accepted: int32 [256], P(('grp', 'seq')), parts along dimension 0, may hold values from 1 to 8
- owner_group: int32 [256], P(('grp', 'seq')), parts along dimension 0, may hold values from 0 to 3, as said below
- page_slot: int32 [256], P(('grp', 'seq')), parts along dimension 0, may hold values from 0 to 63, as said below
Outputs:
- key_cache: bfloat16 [512, 8, 1024], P(('grp', 'seq'), None, 'head'), parts along dimension 0
- value_cache: bfloat16 [512, 8, 1024], P(('grp', 'seq'), None, 'head'), parts along dimension 0
The draws below stay inside these ranges and needn't reach their ends.
There are 2 independent parts, one for each index of `grp`. The reference program is written for one: setup_inputs(seed, part) draws one part's arguments, and reference() takes and returns one part's arrays. A program takes and returns all parts, laid end to end along the dimension named above; an argument that names none is the same for every part. Nothing has to cross between parts.
Inputs may be any that keep to these rules, and one draw needn't show every extreme that they name: `owner_group`: the requests of one index of seq go to exactly 2 distinct owners, 16 to each; some owner receives 64 requests. `page_slot`: the requests of one owner have distinct slots.
All inputs are finite; a program needn't handle non-finite values.
Results may differ from the reference program's by a relative error of at most 0.001.
Values may be sent and summed in bfloat16 or wider, within the bound.
A program may use at most 64 MiB of HBM per device.

```python
import jax
import jax.numpy as jnp

D = 8192
KVH = 8
HD = 128
DRAFT = 8
REQ_DEV = 32
CAP = 16
SLOT_DEV = 64
REQUESTS = 128
ROWS = 1024
N_SEQ = 4


def route_table(key):
    picks = REQ_DEV // CAP
    base = jax.random.fold_in(key, 7)
    key_star, key_scores, key_order, key_pages = jax.random.split(base, 4)
    star = jax.random.randint(key_star, (), 0, N_SEQ)
    scores = jax.vmap(lambda sub: jax.random.permutation(sub, N_SEQ))(jax.random.split(key_scores, N_SEQ))
    scores = jnp.where(jnp.arange(N_SEQ)[None, :] == star, -1, scores)
    ranked = jnp.argsort(scores, axis=1, stable=True).astype(jnp.int32)
    chosen = ranked[:, :picks]
    shuffled = jax.vmap(lambda sub: jax.random.permutation(sub, REQ_DEV))(jax.random.split(key_order, N_SEQ))
    owners = jnp.take_along_axis(chosen, (shuffled // CAP).astype(jnp.int32), axis=1).reshape(-1).astype(jnp.int32)
    priority = jax.random.permutation(key_pages, N_SEQ * REQ_DEV)
    same_owner = owners[:, None] == owners[None, :]
    earlier = priority[None, :] < priority[:, None]
    pages = jnp.sum(jnp.where(same_owner & earlier, 1, 0), axis=1).astype(jnp.int32)
    return (owners, pages)


def draw_owner_group(key, part):
    return route_table(key)[0]


def draw_page_slot(key, part):
    return route_table(key)[1]


def plant(values, rng, low, top_value):
    longest = values.shape.index(max(values.shape))
    spots = []
    for shift in (0, 1):
        where = [jax.random.randint(jax.random.fold_in(rng, axis), (), 0, length) for axis, length in enumerate(values.shape)]
        where[longest] = (where[longest] + shift) % values.shape[longest]
        spots.append(tuple(where))
    return values.at[spots[0]].set(low).at[spots[1]].set(top_value)


def shard_levels(stream_key, extent, pieces, low, high):
    def one(position, parts):
        draws = jax.random.uniform(jax.random.fold_in(jax.random.fold_in(stream_key, 6), position), (parts,), jnp.float32, low / len(pieces), high / len(pieces))
        return jnp.repeat(jnp.exp(draws), extent[position] // parts).reshape((-1,) + (1,) * (len(extent) - position - 1))

    gain = one(*pieces[0])
    for cut in pieces[1:]:
        gain = gain * one(*cut)
    return gain


def noise(stream_key, dims, scale, most, cuts=(), held_as=jnp.bfloat16):
    array = jax.random.normal(stream_key, dims, jnp.float32) * scale
    if len(cuts) > 0:
        array = shard_levels(stream_key, dims, cuts, -0.22, 0.18) * array
    return jnp.clip(array, min=-most, max=most).astype(held_as)


def setup_inputs(seed: int = 0, part: int = 0) -> dict:
    key_of = jax.random.split(jax.random.key(seed), 7)
    own_keys = jax.random.split(jax.random.fold_in(key_of[6], part), 7)
    return {
        "draft_features": noise(own_keys[0], (ROWS, D), 1.0, 6.0, ((0, 4), (1, 4))),
        "w_key": noise(key_of[1], (D, KVH * HD), D ** -0.5, 0.0625, ((1, 4),)),
        "w_value": noise(key_of[2], (D, KVH * HD), D ** -0.5, 0.0625, ((1, 4),)),
        "accepted": plant(jax.random.randint(own_keys[3], (REQUESTS,), 1, DRAFT + 1), jax.random.fold_in(own_keys[3], 1), 1, DRAFT).astype(jnp.int32),
        "owner_group": draw_owner_group(jax.random.fold_in(jax.random.fold_in(key_of[6], part), 71), part),
        "page_slot": draw_page_slot(jax.random.fold_in(jax.random.fold_in(key_of[6], part), 71), part),
    }


def reference(draft_features, w_key, w_value, accepted, owner_group, page_slot):
    key_rows = jnp.dot(draft_features, w_key, preferred_element_type=jnp.float32).astype(jnp.bfloat16)
    value_rows = jnp.dot(draft_features, w_value, preferred_element_type=jnp.float32).astype(jnp.bfloat16)
    live_rows = jnp.arange(DRAFT, dtype=jnp.int32)[None, :] < accepted[:, None]
    key_rows = jnp.where(live_rows[:, :, None], key_rows.reshape(REQUESTS, DRAFT, KVH * HD), jnp.zeros((), key_rows.dtype))
    value_rows = jnp.where(live_rows[:, :, None], value_rows.reshape(REQUESTS, DRAFT, KVH * HD), jnp.zeros((), value_rows.dtype))
    slot_ids = (owner_group * SLOT_DEV + page_slot).astype(jnp.int32)
    key_cache = jnp.zeros((N_SEQ * SLOT_DEV, DRAFT, KVH * HD), key_rows.dtype).at[slot_ids].set(key_rows)
    value_cache = jnp.zeros((N_SEQ * SLOT_DEV, DRAFT, KVH * HD), value_rows.dtype).at[slot_ids].set(value_rows)
    return key_cache, value_cache
```

```python
import functools

import jax
import jax.numpy as jnp
from jax import lax
from jax.experimental import pallas as pl
from jax.experimental.pallas import tpu as pltpu
from jax.sharding import PartitionSpec as P

MESH = pl.DeviceIdType.MESH


def pair_slots(owner_ids, slot_cap):
    row_count = owner_ids.shape[-1]
    same_owner = owner_ids[..., :, None] == owner_ids[..., None, :]
    before = lax.broadcasted_iota(jnp.int32, (row_count, row_count), 1) < lax.broadcasted_iota(
        jnp.int32, (row_count, row_count), 0
    )
    within = jnp.sum(jnp.where(same_owner & before, 1, 0), axis=-1).astype(jnp.int32)
    return owner_ids * slot_cap + within


def one_hot(labels, columns):
    return (
        labels[:, None] == lax.broadcasted_iota(jnp.int32, (labels.shape[0], columns), 1)
    ).astype(jnp.bfloat16)


def pack_rows(payload, slot_ids, slot_total):
    select = one_hot(slot_ids, slot_total)
    packed = lax.dot_general(
        select, payload, (((0,), (0,)), ((), ())), preferred_element_type=jnp.float32
    )
    return packed.astype(jnp.bfloat16)


def placement(all_owner, all_page, owner_self, req_dev, slot_cap, seq_count):
    slot_total = slot_cap * seq_count
    slot_ids = pair_slots(all_owner.reshape(seq_count, req_dev), slot_cap).reshape(-1)
    source = lax.broadcasted_iota(jnp.int32, (seq_count, req_dev), 0).reshape(-1)
    column = source * slot_cap + slot_ids - all_owner * slot_cap
    target = jnp.where(all_owner == owner_self, all_page, -1)
    to_page = one_hot(target, slot_total)
    from_column = one_hot(column, slot_total)
    placing = lax.dot_general(
        to_page, from_column, (((0,), (0,)), ((), ())), preferred_element_type=jnp.float32
    )
    return placing.astype(jnp.bfloat16)


def plain(draft_features, w_key, w_value, accepted, owner_group, page_slot):
    req_dev = accepted.shape[0]
    draft_rows = draft_features.shape[0] // req_dev
    head_cols = w_key.shape[1]
    seq_count = lax.axis_size("seq")
    owner_self = lax.axis_index("seq")
    slot_cap = max(2, 2 * req_dev // seq_count)
    slot_total = slot_cap * seq_count
    send_slots = pair_slots(owner_group, slot_cap)
    live_rows = lax.broadcasted_iota(jnp.int32, (req_dev, draft_rows), 1) < accepted[:, None]
    all_owner, all_page = (
        lax.all_gather(owner_group, "seq", axis=0, tiled=True),
        lax.all_gather(page_slot, "seq", axis=0, tiled=True),
    )
    placing = placement(all_owner, all_page, owner_self, req_dev, slot_cap, seq_count)
    portion = lax.all_gather(draft_features, "head", axis=1, tiled=True)
    key_sum = jnp.dot(portion, w_key, preferred_element_type=jnp.float32)
    value_sum = jnp.dot(portion, w_value, preferred_element_type=jnp.float32)
    key_local = jnp.where(
        live_rows[:, :, None], key_sum.reshape(req_dev, draft_rows, head_cols), 0.0
    )
    value_local = jnp.where(
        live_rows[:, :, None], value_sum.reshape(req_dev, draft_rows, head_cols), 0.0
    )
    key_local = key_local.astype(jnp.bfloat16).reshape(req_dev, draft_rows * head_cols)
    value_local = value_local.astype(jnp.bfloat16).reshape(req_dev, draft_rows * head_cols)
    key_send = pack_rows(key_local, send_slots, slot_total)
    value_send = pack_rows(value_local, send_slots, slot_total)
    key_arrived, value_arrived = (
        lax.all_to_all(key_send, "seq", split_axis=0, concat_axis=0, tiled=True),
        lax.all_to_all(value_send, "seq", split_axis=0, concat_axis=0, tiled=True),
    )
    key_cache = jnp.dot(placing, key_arrived, preferred_element_type=jnp.float32).astype(
        jnp.bfloat16
    )
    value_cache = jnp.dot(placing, value_arrived, preferred_element_type=jnp.float32).astype(
        jnp.bfloat16
    )
    return (
        key_cache.reshape(slot_total, draft_rows, head_cols),
        value_cache.reshape(slot_total, draft_rows, head_cols),
    )


def kernel(
    dims, f_hbm, wk_hbm, wv_hbm, acc_ref, own_ref, page_ref, k_out, v_out,
    feats, weights, part, rows_buf, keys, place, k_stage, v_stage,
    load_sem, w_sem, out_sem, x_send, x_recv, d_send, d_recv, f_send, f_recv,
    z_send, z_recv, i_send, i_recv,
):
    seqs, chunks, draft = dims
    rows, depth = f_hbm.shape
    cols = wk_hbm.shape[1]
    step = rows // chunks
    requests = rows // draft
    slot_rows = k_stage.shape[0]
    head = lax.axis_index("head")
    seq = lax.axis_index("seq")
    partner = head + 1 - 2 * (head % 2)
    across = (head + 2) % 4
    blocks = (head, partner, across, (partner + 2) % 4)

    load = pltpu.make_async_copy(f_hbm, feats.at[0], load_sem)
    load.start()
    w_loads = []
    for k in range(4):
        at = pl.ds(pl.multiple_of(blocks[k] * depth, depth), depth)
        for n, w in enumerate((wk_hbm, wv_hbm)):
            w_loads.append(
                pltpu.make_async_copy(
                    w.at[at, :], weights.at[k, :, pl.ds(n * cols, cols)], w_sem.at[k, n]
                )
            )

    barrier = pltpu.get_barrier_semaphore()
    peers = [{"head": partner}, {"head": across}]
    peers += [{"seq": (seq + d) % seqs} for d in range(1, seqs)]
    for peer in peers:
        pl.semaphore_signal(barrier, inc=1, device_id=peer, device_id_type=MESH)
    for w_load in w_loads:
        w_load.start()
    load.wait()
    pl.semaphore_wait(barrier, len(peers))

    def remote(src, dst, send_sem, recv_sem, peer):
        return pltpu.make_async_remote_copy(
            src_ref=src, dst_ref=dst, send_sem=send_sem, recv_sem=recv_sem,
            device_id=peer, device_id_type=MESH,
        )

    def cut(c):
        return pl.ds(c * step, step)

    def x_copy(c):
        return remote(
            feats.at[0, cut(c), :], feats.at[2, cut(c), :], x_send.at[c], x_recv.at[c],
            {"head": across},
        )

    def forward(c):
        return remote(
            feats.at[2, cut(c), :], feats.at[3, cut(c), :], f_send.at[c], f_recv.at[c],
            {"head": partner},
        )

    def z_copy(c, d):
        return remote(
            rows_buf.at[0, cut(c), :], rows_buf.at[d, cut(c), :],
            z_send.at[d - 1, c], z_recv.at[d - 1, c], {"seq": (seq + d) % seqs},
        )

    def i_copy(d):
        return remote(
            keys.at[0], keys.at[d], i_send.at[d - 1], i_recv.at[d - 1],
            {"seq": (seq + d) % seqs},
        )

    for c in range(chunks):
        x_copy(c).start()
    own = remote(feats.at[0], feats.at[1], d_send, d_recv, {"head": partner})
    own.start()

    spread = (
        lax.broadcasted_iota(jnp.int32, (requests, rows), 1) // draft
        == lax.broadcasted_iota(jnp.int32, (requests, rows), 0)
    ).astype(jnp.bfloat16)

    def widen(ref):
        values = jnp.broadcast_to(ref[...].astype(jnp.float32), (8, requests))
        wide = jnp.dot(
            values.astype(jnp.bfloat16), spread, preferred_element_type=jnp.float32
        )
        return wide.astype(jnp.int32)

    within = lax.broadcasted_iota(jnp.int32, (8, rows), 1) % draft
    keys[0] = jnp.where(
        within < widen(acc_ref),
        widen(own_ref) * slot_rows + widen(page_ref) * draft + within,
        -1,
    )
    for d in range(1, seqs):
        i_copy(d).start()

    w_loads[0].wait()
    w_loads[1].wait()
    part[...] = jnp.dot(feats[0], weights[0], preferred_element_type=jnp.float32)
    own.wait_recv()
    w_loads[2].wait()
    w_loads[3].wait()
    part[...] += jnp.dot(feats[1], weights[1], preferred_element_type=jnp.float32)

    for d in range(seqs):
        if d > 0:
            i_copy(d).wait_recv()
        target = keys[d][0:1, :] - seq * slot_rows
        place[d] = (
            lax.broadcasted_iota(jnp.int32, (slot_rows, rows), 0) == target
        ).astype(jnp.bfloat16)
    for w_load in w_loads[4:]:
        w_load.wait()

    @pl.loop(0, chunks)
    def _(c):
        at = cut(pl.multiple_of(c, 1))
        x_copy(c).wait_recv()
        forward(c).start()
        total = part[at, :] + jnp.dot(
            feats[2, at, :], weights[2], preferred_element_type=jnp.float32
        )
        forward(c).wait_recv()
        total += jnp.dot(feats[3, at, :], weights[3], preferred_element_type=jnp.float32)
        rows_buf[0, at, :] = total.astype(jnp.bfloat16)
        for d in range(1, seqs):
            z_copy(c, d).start()

    half = rows // 2

    def placed(h):
        total = None
        for d in range(seqs):
            more = jnp.dot(
                place[d, :, h * half : (h + 1) * half],
                rows_buf[d, h * half : (h + 1) * half, :],
                preferred_element_type=jnp.float32,
            )
            total = more if total is None else total + more
        return total

    def arrive(first, last):
        @pl.loop(first, last)
        def _(c):
            for d in range(1, seqs):
                z_copy(c, d).wait_recv()

    arrive(0, chunks // 2)
    first = placed(0)
    arrive(chunks // 2, chunks)
    cache = (first + placed(1)).astype(jnp.bfloat16)
    k_stage[...] = cache[:, :cols]
    v_stage[...] = cache[:, cols:]
    outs = [
        pltpu.make_async_copy(k_stage, k_out, out_sem.at[0]),
        pltpu.make_async_copy(v_stage, v_out, out_sem.at[1]),
    ]
    for out in outs:
        out.start()

    @pl.loop(0, chunks)
    def _(c):
        x_copy(c).wait_send()
        forward(c).wait_send()
        for d in range(1, seqs):
            z_copy(c, d).wait_send()

    own.wait_send()
    for d in range(1, seqs):
        i_copy(d).wait_send()
    for out in outs:
        out.wait()


def fused(seqs, draft_features, w_key, w_value, accepted, owner_group, page_slot):
    rows, depth = draft_features.shape
    cols = w_key.shape[1]
    requests = accepted.shape[0]
    draft = rows // requests
    slots = max(2, 2 * requests // seqs) * seqs
    chunks = 8
    step = rows // chunks
    dma = pltpu.SemaphoreType.DMA
    any_spec = pl.BlockSpec(memory_space=pl.ANY)
    vmem_spec = pl.BlockSpec(memory_space=pltpu.VMEM)
    bf16 = jnp.bfloat16
    key_cache, value_cache = pl.pallas_call(
        functools.partial(kernel, (seqs, chunks, draft)),
        out_shape=(jax.ShapeDtypeStruct((slots * draft, cols), bf16),) * 2,
        in_specs=[any_spec] * 3 + [vmem_spec] * 3,
        out_specs=(any_spec, any_spec),
        scratch_shapes=[
            pltpu.VMEM((4, rows, depth), bf16),
            pltpu.VMEM((4, depth, 2 * cols), bf16),
            pltpu.VMEM((rows, 2 * cols), jnp.float32),
            pltpu.VMEM((seqs, rows, 2 * cols), bf16),
            pltpu.VMEM((seqs, 8, rows), jnp.int32),
            pltpu.VMEM((seqs, slots * draft, rows), bf16),
            pltpu.VMEM((slots * draft, cols), bf16),
            pltpu.VMEM((slots * draft, cols), bf16),
            dma, dma((4, 2)), dma((2,)),
            dma((chunks,)), dma((chunks,)), dma, dma, dma((chunks,)), dma((chunks,)),
            dma((seqs - 1, chunks)), dma((seqs - 1, chunks)),
            dma((seqs - 1,)), dma((seqs - 1,)),
        ],
        compiler_params=pltpu.CompilerParams(
            collective_id=0, has_side_effects=True, vmem_limit_bytes=48 << 20
        ),
        name="import_rows",
    )(
        draft_features, w_key, w_value,
        accepted.reshape(1, requests), owner_group.reshape(1, requests),
        page_slot.reshape(1, requests),
    )
    return (
        key_cache.reshape(slots, draft, cols),
        value_cache.reshape(slots, draft, cols),
    )


def solution(mesh):
    placed = (
        P(("grp", "seq"), "head"),
        P(None, "head"),
        P(None, "head"),
        P(("grp", "seq")),
        P(("grp", "seq")),
        P(("grp", "seq")),
    )
    seqs = mesh.shape["seq"]
    local = functools.partial(fused, seqs) if mesh.shape["head"] == 4 else plain
    return jax.shard_map(
        local,
        mesh=mesh,
        in_specs=placed,
        out_specs=(P(("grp", "seq"), None, "head"), P(("grp", "seq"), None, "head")),
        check_vma=False,
    )
```

```python
import functools

import jax
import jax.numpy as jnp
from jax import lax
from jax.experimental import pallas as pl
from jax.experimental.pallas import tpu as pltpu
from jax.sharding import PartitionSpec as P

MESH = pl.DeviceIdType.MESH


def pair_slots(owner_ids, slot_cap):
    row_count = owner_ids.shape[-1]
    same_owner = owner_ids[..., :, None] == owner_ids[..., None, :]
    before = lax.broadcasted_iota(jnp.int32, (row_count, row_count), 1) < lax.broadcasted_iota(
        jnp.int32, (row_count, row_count), 0
    )
    within = jnp.sum(jnp.where(same_owner & before, 1, 0), axis=-1).astype(jnp.int32)
    return owner_ids * slot_cap + within


def one_hot(labels, columns):
    return (
        labels[:, None] == lax.broadcasted_iota(jnp.int32, (labels.shape[0], columns), 1)
    ).astype(jnp.bfloat16)


def pack_rows(payload, slot_ids, slot_total):
    select = one_hot(slot_ids, slot_total)
    packed = lax.dot_general(
        select, payload, (((0,), (0,)), ((), ())), preferred_element_type=jnp.float32
    )
    return packed.astype(jnp.bfloat16)


def placement(all_owner, all_page, owner_self, req_dev, slot_cap, seq_count):
    slot_total = slot_cap * seq_count
    slot_ids = pair_slots(all_owner.reshape(seq_count, req_dev), slot_cap).reshape(-1)
    source = lax.broadcasted_iota(jnp.int32, (seq_count, req_dev), 0).reshape(-1)
    column = source * slot_cap + slot_ids - all_owner * slot_cap
    target = jnp.where(all_owner == owner_self, all_page, -1)
    to_page = one_hot(target, slot_total)
    from_column = one_hot(column, slot_total)
    placing = lax.dot_general(
        to_page, from_column, (((0,), (0,)), ((), ())), preferred_element_type=jnp.float32
    )
    return placing.astype(jnp.bfloat16)


def plain(draft_features, w_key, w_value, accepted, owner_group, page_slot):
    req_dev = accepted.shape[0]
    draft_rows = draft_features.shape[0] // req_dev
    head_cols = w_key.shape[1]
    seq_count = lax.axis_size("seq")
    owner_self = lax.axis_index("seq")
    slot_cap = max(2, 2 * req_dev // seq_count)
    slot_total = slot_cap * seq_count
    send_slots = pair_slots(owner_group, slot_cap)
    live_rows = lax.broadcasted_iota(jnp.int32, (req_dev, draft_rows), 1) < accepted[:, None]
    all_owner, all_page = (
        lax.all_gather(owner_group, "seq", axis=0, tiled=True),
        lax.all_gather(page_slot, "seq", axis=0, tiled=True),
    )
    placing = placement(all_owner, all_page, owner_self, req_dev, slot_cap, seq_count)
    portion = lax.all_gather(draft_features, "head", axis=1, tiled=True)
    key_sum = jnp.dot(portion, w_key, preferred_element_type=jnp.float32)
    value_sum = jnp.dot(portion, w_value, preferred_element_type=jnp.float32)
    key_local = jnp.where(
        live_rows[:, :, None], key_sum.reshape(req_dev, draft_rows, head_cols), 0.0
    )
    value_local = jnp.where(
        live_rows[:, :, None], value_sum.reshape(req_dev, draft_rows, head_cols), 0.0
    )
    key_local = key_local.astype(jnp.bfloat16).reshape(req_dev, draft_rows * head_cols)
    value_local = value_local.astype(jnp.bfloat16).reshape(req_dev, draft_rows * head_cols)
    key_send = pack_rows(key_local, send_slots, slot_total)
    value_send = pack_rows(value_local, send_slots, slot_total)
    key_arrived, value_arrived = (
        lax.all_to_all(key_send, "seq", split_axis=0, concat_axis=0, tiled=True),
        lax.all_to_all(value_send, "seq", split_axis=0, concat_axis=0, tiled=True),
    )
    key_cache = jnp.dot(placing, key_arrived, preferred_element_type=jnp.float32).astype(
        jnp.bfloat16
    )
    value_cache = jnp.dot(placing, value_arrived, preferred_element_type=jnp.float32).astype(
        jnp.bfloat16
    )
    return (
        key_cache.reshape(slot_total, draft_rows, head_cols),
        value_cache.reshape(slot_total, draft_rows, head_cols),
    )


def kernel(
    dims, f_hbm, wk_hbm, wv_hbm, acc_hbm, own_hbm, page_hbm, k_out, v_out,
    feats, weights, part, rows_buf, keys, place, acc_ref, own_ref, page_ref,
    load_sem, w_sem, id_sem, x_send, x_recv, d_send, d_recv, f_send, f_recv,
    z_send, z_recv, i_send, i_recv,
):
    seqs, chunks, draft = dims
    rows, depth = f_hbm.shape
    cols = wk_hbm.shape[1]
    step = rows // chunks
    requests = rows // draft
    slot_rows = k_out.shape[0]
    head = lax.axis_index("head")
    seq = lax.axis_index("seq")
    partner = head + 1 - 2 * (head % 2)
    across = (head + 2) % 4
    blocks = (head, partner, across, (partner + 2) % 4)

    load = pltpu.make_async_copy(f_hbm, feats.at[0], load_sem)
    load.start()
    id_loads = [
        pltpu.make_async_copy(src, dst, id_sem.at[n])
        for n, (src, dst) in enumerate(
            ((acc_hbm, acc_ref), (own_hbm, own_ref), (page_hbm, page_ref))
        )
    ]
    for id_load in id_loads:
        id_load.start()
    w_loads = []
    for k in range(4):
        at = pl.ds(pl.multiple_of(blocks[k] * depth, depth), depth)
        for n, w in enumerate((wk_hbm, wv_hbm)):
            w_loads.append(
                pltpu.make_async_copy(
                    w.at[at, :], weights.at[k, :, pl.ds(n * cols, cols)], w_sem.at[k, n]
                )
            )

    barrier = pltpu.get_barrier_semaphore()
    peers = [{"head": partner}, {"head": across}]
    peers += [{"seq": (seq + d) % seqs} for d in range(1, seqs)]
    for peer in peers:
        pl.semaphore_signal(barrier, inc=1, device_id=peer, device_id_type=MESH)
    for w_load in w_loads:
        w_load.start()
    load.wait()
    pl.semaphore_wait(barrier, len(peers))

    def remote(src, dst, send_sem, recv_sem, peer):
        return pltpu.make_async_remote_copy(
            src_ref=src, dst_ref=dst, send_sem=send_sem, recv_sem=recv_sem,
            device_id=peer, device_id_type=MESH,
        )

    def cut(c):
        return pl.ds(c * step, step)

    def x_copy(c):
        return remote(
            feats.at[0, cut(c), :], feats.at[2, cut(c), :], x_send.at[c], x_recv.at[c],
            {"head": across},
        )

    def forward(c):
        return remote(
            feats.at[2, cut(c), :], feats.at[3, cut(c), :], f_send.at[c], f_recv.at[c],
            {"head": partner},
        )

    def z_copy(c, d):
        return remote(
            rows_buf.at[0, cut(c), :], rows_buf.at[d, cut(c), :],
            z_send.at[d - 1, c], z_recv.at[d - 1, c], {"seq": (seq + d) % seqs},
        )

    def i_copy(d):
        return remote(
            keys.at[0], keys.at[d], i_send.at[d - 1], i_recv.at[d - 1],
            {"seq": (seq + d) % seqs},
        )

    for c in range(chunks):
        x_copy(c).start()
    own = remote(feats.at[0], feats.at[1], d_send, d_recv, {"head": partner})
    own.start()

    for id_load in id_loads:
        id_load.wait()
    spread = (
        lax.broadcasted_iota(jnp.int32, (requests, rows), 1) // draft
        == lax.broadcasted_iota(jnp.int32, (requests, rows), 0)
    ).astype(jnp.bfloat16)

    def widen(ref):
        values = jnp.broadcast_to(ref[...].astype(jnp.float32), (8, requests))
        wide = jnp.dot(
            values.astype(jnp.bfloat16), spread, preferred_element_type=jnp.float32
        )
        return wide.astype(jnp.int32)

    within = lax.broadcasted_iota(jnp.int32, (8, rows), 1) % draft
    keys[0] = jnp.where(
        within < widen(acc_ref),
        widen(own_ref) * slot_rows + widen(page_ref) * draft + within,
        -1,
    )
    for d in range(1, seqs):
        i_copy(d).start()

    w_loads[0].wait()
    w_loads[1].wait()
    part[...] = jnp.dot(feats[0], weights[0], preferred_element_type=jnp.float32)
    own.wait_recv()
    w_loads[2].wait()
    w_loads[3].wait()
    part[...] += jnp.dot(feats[1], weights[1], preferred_element_type=jnp.float32)

    for d in range(seqs):
        if d > 0:
            i_copy(d).wait_recv()
        target = keys[d][0:1, :] - seq * slot_rows
        place[d] = (
            lax.broadcasted_iota(jnp.int32, (slot_rows, rows), 0) == target
        ).astype(jnp.bfloat16)
    for w_load in w_loads[4:]:
        w_load.wait()

    @pl.loop(0, chunks)
    def _(c):
        at = cut(pl.multiple_of(c, 1))
        x_copy(c).wait_recv()
        forward(c).start()
        total = part[at, :] + jnp.dot(
            feats[2, at, :], weights[2], preferred_element_type=jnp.float32
        )
        forward(c).wait_recv()
        total += jnp.dot(feats[3, at, :], weights[3], preferred_element_type=jnp.float32)
        rows_buf[0, at, :] = total.astype(jnp.bfloat16)
        for d in range(1, seqs):
            z_copy(c, d).start()

    half = rows // 2

    def placed(h):
        total = None
        for d in range(seqs):
            more = jnp.dot(
                place[d, :, h * half : (h + 1) * half],
                rows_buf[d, h * half : (h + 1) * half, :],
                preferred_element_type=jnp.float32,
            )
            total = more if total is None else total + more
        return total

    def arrive(first, last):
        @pl.loop(first, last)
        def _(c):
            for d in range(1, seqs):
                z_copy(c, d).wait_recv()

    arrive(0, chunks // 2)
    first = placed(0)
    arrive(chunks // 2, chunks)
    cache = (first + placed(1)).astype(jnp.bfloat16)
    k_out[...] = cache[:, :cols]
    v_out[...] = cache[:, cols:]

    @pl.loop(0, chunks)
    def _(c):
        x_copy(c).wait_send()
        forward(c).wait_send()
        for d in range(1, seqs):
            z_copy(c, d).wait_send()

    own.wait_send()
    for d in range(1, seqs):
        i_copy(d).wait_send()


def fused(seqs, draft_features, w_key, w_value, accepted, owner_group, page_slot):
    rows, depth = draft_features.shape
    cols = w_key.shape[1]
    requests = accepted.shape[0]
    draft = rows // requests
    slots = max(2, 2 * requests // seqs) * seqs
    chunks = 8
    step = rows // chunks
    dma = pltpu.SemaphoreType.DMA
    hbm_spec = pl.BlockSpec(memory_space=pltpu.HBM)
    vmem_spec = pl.BlockSpec(memory_space=pltpu.VMEM)
    bf16 = jnp.bfloat16
    key_cache, value_cache = pl.pallas_call(
        functools.partial(kernel, (seqs, chunks, draft)),
        out_shape=(jax.ShapeDtypeStruct((slots * draft, cols), bf16),) * 2,
        in_specs=[hbm_spec] * 6,
        out_specs=(vmem_spec, vmem_spec),
        scratch_shapes=[
            pltpu.VMEM((4, rows, depth), bf16),
            pltpu.VMEM((4, depth, 2 * cols), bf16),
            pltpu.VMEM((rows, 2 * cols), jnp.float32),
            pltpu.VMEM((seqs, rows, 2 * cols), bf16),
            pltpu.VMEM((seqs, 8, rows), jnp.int32),
            pltpu.VMEM((seqs, slots * draft, rows), bf16),
            pltpu.VMEM((1, requests), jnp.int32),
            pltpu.VMEM((1, requests), jnp.int32),
            pltpu.VMEM((1, requests), jnp.int32),
            dma, dma((4, 2)), dma((3,)),
            dma((chunks,)), dma((chunks,)), dma, dma, dma((chunks,)), dma((chunks,)),
            dma((seqs - 1, chunks)), dma((seqs - 1, chunks)),
            dma((seqs - 1,)), dma((seqs - 1,)),
        ],
        compiler_params=pltpu.CompilerParams(
            collective_id=0, has_side_effects=True, vmem_limit_bytes=67043328
        ),
        name="import_rows",
    )(
        draft_features, w_key, w_value,
        accepted.reshape(1, requests), owner_group.reshape(1, requests),
        page_slot.reshape(1, requests),
    )
    return (
        key_cache.reshape(slots, draft, cols),
        value_cache.reshape(slots, draft, cols),
    )


def solution(mesh):
    placed = (
        P(("grp", "seq"), "head"),
        P(None, "head"),
        P(None, "head"),
        P(("grp", "seq")),
        P(("grp", "seq")),
        P(("grp", "seq")),
    )
    seqs = mesh.shape["seq"]
    local = functools.partial(fused, seqs) if mesh.shape["head"] == 4 else plain
    return jax.shard_map(
        local,
        mesh=mesh,
        in_specs=placed,
        out_specs=(P(("grp", "seq"), None, "head"), P(("grp", "seq"), None, "head")),
        check_vma=False,
    )
```

```python
import functools

import jax
import jax.numpy as jnp
from jax import lax
from jax.experimental import pallas as pl
from jax.experimental.pallas import tpu as pltpu
from jax.sharding import PartitionSpec as P

MESH = pl.DeviceIdType.MESH


def pair_slots(owner_ids, slot_cap):
    row_count = owner_ids.shape[-1]
    same_owner = owner_ids[..., :, None] == owner_ids[..., None, :]
    before = lax.broadcasted_iota(jnp.int32, (row_count, row_count), 1) < lax.broadcasted_iota(
        jnp.int32, (row_count, row_count), 0
    )
    within = jnp.sum(jnp.where(same_owner & before, 1, 0), axis=-1).astype(jnp.int32)
    return owner_ids * slot_cap + within


def one_hot(labels, columns):
    return (
        labels[:, None] == lax.broadcasted_iota(jnp.int32, (labels.shape[0], columns), 1)
    ).astype(jnp.bfloat16)


def pack_rows(payload, slot_ids, slot_total):
    select = one_hot(slot_ids, slot_total)
    packed = lax.dot_general(
        select, payload, (((0,), (0,)), ((), ())), preferred_element_type=jnp.float32
    )
    return packed.astype(jnp.bfloat16)


def placement(all_owner, all_page, owner_self, req_dev, slot_cap, seq_count):
    slot_total = slot_cap * seq_count
    slot_ids = pair_slots(all_owner.reshape(seq_count, req_dev), slot_cap).reshape(-1)
    source = lax.broadcasted_iota(jnp.int32, (seq_count, req_dev), 0).reshape(-1)
    column = source * slot_cap + slot_ids - all_owner * slot_cap
    target = jnp.where(all_owner == owner_self, all_page, -1)
    to_page = one_hot(target, slot_total)
    from_column = one_hot(column, slot_total)
    placing = lax.dot_general(
        to_page, from_column, (((0,), (0,)), ((), ())), preferred_element_type=jnp.float32
    )
    return placing.astype(jnp.bfloat16)


def plain(draft_features, w_key, w_value, accepted, owner_group, page_slot):
    req_dev = accepted.shape[0]
    draft_rows = draft_features.shape[0] // req_dev
    head_cols = w_key.shape[1]
    seq_count = lax.axis_size("seq")
    owner_self = lax.axis_index("seq")
    slot_cap = max(2, 2 * req_dev // seq_count)
    slot_total = slot_cap * seq_count
    send_slots = pair_slots(owner_group, slot_cap)
    live_rows = lax.broadcasted_iota(jnp.int32, (req_dev, draft_rows), 1) < accepted[:, None]
    all_owner, all_page = (
        lax.all_gather(owner_group, "seq", axis=0, tiled=True),
        lax.all_gather(page_slot, "seq", axis=0, tiled=True),
    )
    placing = placement(all_owner, all_page, owner_self, req_dev, slot_cap, seq_count)
    portion = lax.all_gather(draft_features, "head", axis=1, tiled=True)
    key_sum = jnp.dot(portion, w_key, preferred_element_type=jnp.float32)
    value_sum = jnp.dot(portion, w_value, preferred_element_type=jnp.float32)
    key_local = jnp.where(
        live_rows[:, :, None], key_sum.reshape(req_dev, draft_rows, head_cols), 0.0
    )
    value_local = jnp.where(
        live_rows[:, :, None], value_sum.reshape(req_dev, draft_rows, head_cols), 0.0
    )
    key_local = key_local.astype(jnp.bfloat16).reshape(req_dev, draft_rows * head_cols)
    value_local = value_local.astype(jnp.bfloat16).reshape(req_dev, draft_rows * head_cols)
    key_send = pack_rows(key_local, send_slots, slot_total)
    value_send = pack_rows(value_local, send_slots, slot_total)
    key_arrived, value_arrived = (
        lax.all_to_all(key_send, "seq", split_axis=0, concat_axis=0, tiled=True),
        lax.all_to_all(value_send, "seq", split_axis=0, concat_axis=0, tiled=True),
    )
    key_cache = jnp.dot(placing, key_arrived, preferred_element_type=jnp.float32).astype(
        jnp.bfloat16
    )
    value_cache = jnp.dot(placing, value_arrived, preferred_element_type=jnp.float32).astype(
        jnp.bfloat16
    )
    return (
        key_cache.reshape(slot_total, draft_rows, head_cols),
        value_cache.reshape(slot_total, draft_rows, head_cols),
    )


def kernel(
    dims, f_hbm, wk_hbm, wv_hbm, acc_hbm, own_hbm, page_hbm, k_out, v_out,
    raw, feats, weights, part, z_out, z_in, key_out, key_in, place,
    acc_ref, own_ref, page_ref,
    load_sem, w_sem, id_sem, x_send, x_recv, d_send, d_recv, f_send, f_recv,
    z_send, z_recv, i_send, i_recv,
):
    seqs, chunks, draft = dims
    rows, depth = f_hbm.shape
    cols = wk_hbm.shape[1]
    step = rows // chunks
    requests = rows // draft
    cap = requests // 2
    share = cap // chunks
    piece = share * draft
    slot_rows = k_out.shape[0]
    bf16, f32, i32 = jnp.bfloat16, jnp.float32, jnp.int32
    head = lax.axis_index("head")
    seq = lax.axis_index("seq")
    partner = head + 1 - 2 * (head % 2)
    across = (head + 2) % 4
    blocks = (head, partner, across, (partner + 2) % 4)

    id_loads = [
        pltpu.make_async_copy(src, dst, id_sem.at[n])
        for n, (src, dst) in enumerate(
            ((own_hbm, own_ref), (acc_hbm, acc_ref), (page_hbm, page_ref))
        )
    ]
    for id_load in id_loads:
        id_load.start()
    load = pltpu.make_async_copy(f_hbm, raw, load_sem)
    load.start()
    w_loads = []
    for k in range(4):
        at = pl.ds(pl.multiple_of(blocks[k] * depth, depth), depth)
        for n, w in enumerate((wk_hbm, wv_hbm)):
            w_loads.append(
                pltpu.make_async_copy(
                    w.at[at, :], weights.at[k, :, pl.ds(n * cols, cols)], w_sem.at[k, n]
                )
            )

    barrier = pltpu.get_barrier_semaphore()
    peers = [{"head": partner}, {"head": across}]
    peers += [{"seq": (seq + d) % seqs} for d in range(1, seqs)]
    for peer in peers:
        pl.semaphore_signal(barrier, inc=1, device_id=peer, device_id_type=MESH)
    for w_load in w_loads:
        w_load.start()

    def iota(shape, dim):
        return lax.broadcasted_iota(i32, shape, dim)

    def exact(values, table, dims=(((1,), (0,)), ((), ()))):
        return lax.dot_general(
            values.astype(bf16), table.astype(bf16), dims, preferred_element_type=f32
        )

    for id_load in id_loads:
        id_load.wait()
    owner = own_ref[...]
    low = jnp.min(owner, axis=1, keepdims=True)
    high = jnp.max(owner, axis=1, keepdims=True)
    mine = (iota((8, requests), 0) == owner).astype(f32)
    earlier = (iota((requests, requests), 0) < iota((requests, requests), 1)).astype(f32)
    rank = jnp.sum(mine * exact(mine, earlier), axis=0, keepdims=True).astype(i32)
    spot = (rank // share) * (2 * share) + rank % share + jnp.where(owner > low, share, 0)
    spread = (iota((requests, rows), 1) // draft == iota((requests, rows), 0)).astype(f32)
    wide = exact(jnp.broadcast_to(spot.astype(f32), (8, requests)), spread)
    goal = wide.astype(i32)[0:1, :] * draft + iota((1, rows), 1) % draft
    order = (iota((rows, rows), 0) == goal).astype(bf16)

    load.wait()
    pl.semaphore_wait(barrier, len(peers))

    def remote(src, dst, send_sem, recv_sem, peer):
        return pltpu.make_async_remote_copy(
            src_ref=src, dst_ref=dst, send_sem=send_sem, recv_sem=recv_sem,
            device_id=peer, device_id_type=MESH,
        )

    def cut(c):
        return pl.ds(c * step, step)

    def x_copy(c):
        return remote(
            feats.at[0, cut(c), :], feats.at[2, cut(c), :], x_send.at[c], x_recv.at[c],
            {"head": across},
        )

    def forward(c):
        return remote(
            feats.at[2, cut(c), :], feats.at[3, cut(c), :], f_send.at[c], f_recv.at[c],
            {"head": partner},
        )

    def z_copy(c, d):
        at = pl.ds(c * piece, piece)
        return remote(
            z_out.at[d - 1, at, :], z_in.at[d, at, :],
            z_send.at[d - 1, c], z_recv.at[d - 1, c], {"seq": (seq + d) % seqs},
        )

    def i_copy(d):
        return remote(
            key_out.at[d - 1], key_in.at[d], i_send.at[d - 1], i_recv.at[d - 1],
            {"seq": (seq + d) % seqs},
        )

    early = 2
    for first, last in ((0, early), (early, chunks)):
        some = slice(first * step, last * step)
        feats[0, some, :] = jnp.dot(
            order[some], raw[...], preferred_element_type=f32
        ).astype(bf16)
        for c in range(first, last):
            x_copy(c).start()
    own = remote(feats.at[0], feats.at[1], d_send, d_recv, {"head": partner})
    own.start()

    page = jnp.broadcast_to(page_ref[...].astype(f32), (8, requests))
    live = jnp.broadcast_to(acc_ref[...].astype(f32), (8, requests))
    within = iota((8, cap * draft), 1) % draft
    last_dims = (((1,), (1,)), ((), ()))
    for d in range(seqs):
        taken = (
            (owner == (seq + d) % seqs) & (rank == iota((cap * draft, requests), 0) // draft)
        ).astype(f32)
        key = jnp.where(
            within < exact(live, taken, last_dims).astype(i32),
            exact(page, taken, last_dims).astype(i32) * draft + within,
            -1,
        )
        if d == 0:
            key_in[0] = key
        else:
            key_out[d - 1] = key
            i_copy(d).start()

    w_loads[0].wait()
    w_loads[1].wait()
    part[...] = jnp.dot(feats[0], weights[0], preferred_element_type=f32)
    own.wait_recv()
    w_loads[2].wait()
    w_loads[3].wait()
    part[...] += jnp.dot(feats[1], weights[1], preferred_element_type=f32)

    for d in range(seqs):
        if d > 0:
            i_copy(d).wait_recv()
        place[:, d * cap * draft : (d + 1) * cap * draft] = (
            iota((slot_rows, cap * draft), 0) == key_in[d][0:1, :]
        ).astype(bf16)
    for w_load in w_loads[4:]:
        w_load.wait()

    @pl.loop(0, chunks)
    def _(c):
        at = cut(c)
        x_copy(c).wait_recv()
        forward(c).start()
        total = part[at, :] + jnp.dot(
            feats[2, at, :], weights[2], preferred_element_type=f32
        )
        forward(c).wait_recv()
        total += jnp.dot(feats[3, at, :], weights[3], preferred_element_type=f32)
        of_low, of_high = total[:piece], total[piece:]
        to = pl.ds(c * piece, piece)
        for d in [*range(1, seqs), 0]:
            target = (seq + d) % seqs
            chosen = jnp.where(
                low == target, of_low, jnp.where(high == target, of_high, 0.0)
            ).astype(bf16)
            if d == 0:
                z_in[0, to, :] = chosen
            else:
                z_out[d - 1, to, :] = chosen
                z_copy(c, d).start()

    @pl.loop(0, chunks)
    def _(c):
        for d in range(1, seqs):
            z_copy(c, d).wait_recv()

    arrived = z_in[...].reshape(seqs * cap * draft, 2 * cols)
    cache = jnp.dot(place[...], arrived, preferred_element_type=f32).astype(bf16)
    k_out[...] = cache[:, :cols]
    v_out[...] = cache[:, cols:]

    @pl.loop(0, chunks)
    def _(c):
        x_copy(c).wait_send()
        forward(c).wait_send()
        for d in range(1, seqs):
            z_copy(c, d).wait_send()

    own.wait_send()
    for d in range(1, seqs):
        i_copy(d).wait_send()


def fused(seqs, draft_features, w_key, w_value, accepted, owner_group, page_slot):
    rows, depth = draft_features.shape
    cols = w_key.shape[1]
    requests = accepted.shape[0]
    draft = rows // requests
    slots = max(2, 2 * requests // seqs) * seqs
    chunks = 8
    sent = rows // 2
    if 2 * (slots // seqs) != requests:
        return plain(draft_features, w_key, w_value, accepted, owner_group, page_slot)
    dma = pltpu.SemaphoreType.DMA
    hbm_spec = pl.BlockSpec(memory_space=pltpu.HBM)
    vmem_spec = pl.BlockSpec(memory_space=pltpu.VMEM)
    bf16 = jnp.bfloat16
    key_cache, value_cache = pl.pallas_call(
        functools.partial(kernel, (seqs, chunks, draft)),
        out_shape=(jax.ShapeDtypeStruct((slots * draft, cols), bf16),) * 2,
        in_specs=[hbm_spec] * 6,
        out_specs=(vmem_spec, vmem_spec),
        scratch_shapes=[
            pltpu.VMEM((rows, depth), bf16),
            pltpu.VMEM((4, rows, depth), bf16),
            pltpu.VMEM((4, depth, 2 * cols), bf16),
            pltpu.VMEM((rows, 2 * cols), jnp.float32),
            pltpu.VMEM((seqs - 1, sent, 2 * cols), bf16),
            pltpu.VMEM((seqs, sent, 2 * cols), bf16),
            pltpu.VMEM((seqs - 1, 8, sent), jnp.int32),
            pltpu.VMEM((seqs, 8, sent), jnp.int32),
            pltpu.VMEM((slots * draft, seqs * sent), bf16),
            pltpu.VMEM((1, requests), jnp.int32),
            pltpu.VMEM((1, requests), jnp.int32),
            pltpu.VMEM((1, requests), jnp.int32),
            dma, dma((4, 2)), dma((3,)),
            dma((chunks,)), dma((chunks,)), dma, dma, dma((chunks,)), dma((chunks,)),
            dma((seqs - 1, chunks)), dma((seqs - 1, chunks)),
            dma((seqs - 1,)), dma((seqs - 1,)),
        ],
        compiler_params=pltpu.CompilerParams(
            collective_id=0, has_side_effects=True, vmem_limit_bytes=48 << 20
        ),
        name="import_rows",
    )(
        *(
            pltpu.with_memory_space_constraint(x, pltpu.HBM)
            for x in (
                draft_features, w_key, w_value,
                accepted.reshape(1, requests), owner_group.reshape(1, requests),
                page_slot.reshape(1, requests),
            )
        )
    )
    return (
        key_cache.reshape(slots, draft, cols),
        value_cache.reshape(slots, draft, cols),
    )


def solution(mesh):
    placed = (
        P(("grp", "seq"), "head"),
        P(None, "head"),
        P(None, "head"),
        P(("grp", "seq")),
        P(("grp", "seq")),
        P(("grp", "seq")),
    )
    seqs = mesh.shape["seq"]
    local = functools.partial(fused, seqs) if mesh.shape["head"] == 4 else plain
    return jax.shard_map(
        local,
        mesh=mesh,
        in_specs=placed,
        out_specs=(P(("grp", "seq"), None, "head"), P(("grp", "seq"), None, "head")),
        check_vma=False,
    )
```

```python
import functools

import jax
import jax.numpy as jnp
from jax import lax
from jax.experimental import pallas as pl
from jax.experimental.pallas import tpu as pltpu
from jax.sharding import PartitionSpec as P

MESH = pl.DeviceIdType.MESH


def pair_slots(owner_ids, slot_cap):
    row_count = owner_ids.shape[-1]
    same_owner = owner_ids[..., :, None] == owner_ids[..., None, :]
    before = lax.broadcasted_iota(jnp.int32, (row_count, row_count), 1) < lax.broadcasted_iota(
        jnp.int32, (row_count, row_count), 0
    )
    within = jnp.sum(jnp.where(same_owner & before, 1, 0), axis=-1).astype(jnp.int32)
    return owner_ids * slot_cap + within


def one_hot(labels, columns):
    return (
        labels[:, None] == lax.broadcasted_iota(jnp.int32, (labels.shape[0], columns), 1)
    ).astype(jnp.bfloat16)


def pack_rows(payload, slot_ids, slot_total):
    select = one_hot(slot_ids, slot_total)
    packed = lax.dot_general(
        select, payload, (((0,), (0,)), ((), ())), preferred_element_type=jnp.float32
    )
    return packed.astype(jnp.bfloat16)


def placement(all_owner, all_page, owner_self, req_dev, slot_cap, seq_count):
    slot_total = slot_cap * seq_count
    slot_ids = pair_slots(all_owner.reshape(seq_count, req_dev), slot_cap).reshape(-1)
    source = lax.broadcasted_iota(jnp.int32, (seq_count, req_dev), 0).reshape(-1)
    column = source * slot_cap + slot_ids - all_owner * slot_cap
    target = jnp.where(all_owner == owner_self, all_page, -1)
    to_page = one_hot(target, slot_total)
    from_column = one_hot(column, slot_total)
    placing = lax.dot_general(
        to_page, from_column, (((0,), (0,)), ((), ())), preferred_element_type=jnp.float32
    )
    return placing.astype(jnp.bfloat16)


def plain(draft_features, w_key, w_value, accepted, owner_group, page_slot):
    req_dev = accepted.shape[0]
    draft_rows = draft_features.shape[0] // req_dev
    head_cols = w_key.shape[1]
    seq_count = lax.axis_size("seq")
    owner_self = lax.axis_index("seq")
    slot_cap = max(2, 2 * req_dev // seq_count)
    slot_total = slot_cap * seq_count
    send_slots = pair_slots(owner_group, slot_cap)
    live_rows = lax.broadcasted_iota(jnp.int32, (req_dev, draft_rows), 1) < accepted[:, None]
    all_owner, all_page = (
        lax.all_gather(owner_group, "seq", axis=0, tiled=True),
        lax.all_gather(page_slot, "seq", axis=0, tiled=True),
    )
    placing = placement(all_owner, all_page, owner_self, req_dev, slot_cap, seq_count)
    portion = lax.all_gather(draft_features, "head", axis=1, tiled=True)
    key_sum = jnp.dot(portion, w_key, preferred_element_type=jnp.float32)
    value_sum = jnp.dot(portion, w_value, preferred_element_type=jnp.float32)
    key_local = jnp.where(
        live_rows[:, :, None], key_sum.reshape(req_dev, draft_rows, head_cols), 0.0
    )
    value_local = jnp.where(
        live_rows[:, :, None], value_sum.reshape(req_dev, draft_rows, head_cols), 0.0
    )
    key_local = key_local.astype(jnp.bfloat16).reshape(req_dev, draft_rows * head_cols)
    value_local = value_local.astype(jnp.bfloat16).reshape(req_dev, draft_rows * head_cols)
    key_send = pack_rows(key_local, send_slots, slot_total)
    value_send = pack_rows(value_local, send_slots, slot_total)
    key_arrived, value_arrived = (
        lax.all_to_all(key_send, "seq", split_axis=0, concat_axis=0, tiled=True),
        lax.all_to_all(value_send, "seq", split_axis=0, concat_axis=0, tiled=True),
    )
    key_cache = jnp.dot(placing, key_arrived, preferred_element_type=jnp.float32).astype(
        jnp.bfloat16
    )
    value_cache = jnp.dot(placing, value_arrived, preferred_element_type=jnp.float32).astype(
        jnp.bfloat16
    )
    return (
        key_cache.reshape(slot_total, draft_rows, head_cols),
        value_cache.reshape(slot_total, draft_rows, head_cols),
    )


def kernel(
    dims, f_hbm, wk_hbm, wv_hbm, acc_hbm, own_hbm, page_hbm, k_out, v_out,
    raw, feats, weights, part, z_out, z_in, key_out, key_in, place, cache,
    acc_ref, own_ref, page_ref,
    load_sem, w_sem, id_sem, x_send, x_recv, d_send, d_recv, f_send, f_recv,
    z_send, z_recv, i_send, i_recv,
):
    seqs, chunks, draft = dims
    rows, depth = f_hbm.shape
    cols = wk_hbm.shape[1]
    step = rows // chunks
    requests = rows // draft
    cap = requests // 2
    share = cap // chunks
    piece = share * draft
    group = cap * draft // 2
    turns = chunks // 2
    slot_rows = k_out.shape[0]
    bf16, f32, i32 = jnp.bfloat16, jnp.float32, jnp.int32
    head = lax.axis_index("head")
    seq = lax.axis_index("seq")
    partner = head + 1 - 2 * (head % 2)
    across = (head + 2) % 4
    blocks = (head, partner, across, (partner + 2) % 4)

    id_loads = [
        pltpu.make_async_copy(src, dst, id_sem.at[n])
        for n, (src, dst) in enumerate(
            ((own_hbm, own_ref), (acc_hbm, acc_ref), (page_hbm, page_ref))
        )
    ]
    for id_load in id_loads:
        id_load.start()
    load = pltpu.make_async_copy(f_hbm, raw, load_sem)
    load.start()
    w_loads = []
    for k in range(4):
        at = pl.ds(pl.multiple_of(blocks[k] * depth, depth), depth)
        for n, w in enumerate((wk_hbm, wv_hbm)):
            w_loads.append(
                pltpu.make_async_copy(
                    w.at[at, :], weights.at[k, :, pl.ds(n * cols, cols)], w_sem.at[k, n]
                )
            )

    barrier = pltpu.get_barrier_semaphore()
    peers = [{"head": partner}, {"head": across}]
    peers += [{"seq": (seq + d) % seqs} for d in range(1, seqs)]
    for peer in peers:
        pl.semaphore_signal(barrier, inc=1, device_id=peer, device_id_type=MESH)
    for w_load in w_loads:
        w_load.start()

    def iota(shape, dim):
        return lax.broadcasted_iota(i32, shape, dim)

    def exact(values, table, dims=(((1,), (0,)), ((), ()))):
        return lax.dot_general(
            values.astype(bf16), table.astype(bf16), dims, preferred_element_type=f32
        )

    for id_load in id_loads:
        id_load.wait()
    owner = own_ref[...]
    low = jnp.min(owner, axis=1, keepdims=True)
    high = jnp.max(owner, axis=1, keepdims=True)
    mine = (iota((8, requests), 0) == owner).astype(f32)
    earlier = (iota((requests, requests), 0) < iota((requests, requests), 1)).astype(f32)
    rank = jnp.sum(mine * exact(mine, earlier), axis=0, keepdims=True).astype(i32)
    spot = (rank // share) * (2 * share) + rank % share + jnp.where(owner > low, share, 0)
    spread = (iota((requests, rows), 1) // draft == iota((requests, rows), 0)).astype(f32)
    wide = exact(jnp.broadcast_to(spot.astype(f32), (8, requests)), spread)
    goal = wide.astype(i32)[0:1, :] * draft + iota((1, rows), 1) % draft
    order = (iota((rows, rows), 0) == goal).astype(bf16)

    load.wait()

    def remote(src, dst, send_sem, recv_sem, peer):
        return pltpu.make_async_remote_copy(
            src_ref=src, dst_ref=dst, send_sem=send_sem, recv_sem=recv_sem,
            device_id=peer, device_id_type=MESH,
        )

    def cut(c):
        return pl.ds(c * step, step)

    def x_copy(c):
        return remote(
            feats.at[0, cut(c), :], feats.at[2, cut(c), :], x_send.at[c], x_recv.at[c],
            {"head": across},
        )

    def forward(c):
        return remote(
            feats.at[2, cut(c), :], feats.at[3, cut(c), :], f_send.at[c], f_recv.at[c],
            {"head": partner},
        )

    def z_copy(c, d):
        at = pl.ds(c * piece, piece)
        there = pl.ds((c % turns) * piece, piece)
        return remote(
            z_out.at[d - 1, at, :], z_in.at[c // turns, d, there, :],
            z_send.at[d - 1, c], z_recv.at[d - 1, c], {"seq": (seq + d) % seqs},
        )

    def i_copy(d):
        return remote(
            key_out.at[d - 1], key_in.at[d], i_send.at[d - 1], i_recv.at[d - 1],
            {"seq": (seq + d) % seqs},
        )

    early = 2
    for first, last in ((0, early), (early, chunks)):
        some = slice(first * step, last * step)
        feats[0, some, :] = jnp.dot(
            order[some], raw[...], preferred_element_type=f32
        ).astype(bf16)
        if first == 0:
            pl.semaphore_wait(barrier, len(peers))
        for c in range(first, last):
            x_copy(c).start()
    own = remote(feats.at[0], feats.at[1], d_send, d_recv, {"head": partner})
    own.start()

    page = jnp.broadcast_to(page_ref[...].astype(f32), (8, requests))
    live = jnp.broadcast_to(acc_ref[...].astype(f32), (8, requests))
    within = iota((8, cap * draft), 1) % draft
    last_dims = (((1,), (1,)), ((), ()))
    for d in range(seqs):
        taken = (
            (owner == (seq + d) % seqs) & (rank == iota((cap * draft, requests), 0) // draft)
        ).astype(f32)
        key = jnp.where(
            within < exact(live, taken, last_dims).astype(i32),
            exact(page, taken, last_dims).astype(i32) * draft + within,
            -1,
        )
        if d == 0:
            key_in[0] = key
        else:
            key_out[d - 1] = key
            i_copy(d).start()

    w_loads[0].wait()
    w_loads[1].wait()
    part[...] = jnp.dot(feats[0], weights[0], preferred_element_type=f32)
    own.wait_recv()
    w_loads[2].wait()
    w_loads[3].wait()
    part[...] += jnp.dot(feats[1], weights[1], preferred_element_type=f32)

    for d in range(seqs):
        if d > 0:
            i_copy(d).wait_recv()
        placing = (iota((slot_rows, cap * draft), 0) == key_in[d][0:1, :]).astype(bf16)
        for g in range(2):
            place[g, :, d * group : (d + 1) * group] = placing[:, g * group : (g + 1) * group]
    for w_load in w_loads[4:]:
        w_load.wait()

    def meet(c):
        x_copy(c).wait_recv()
        forward(c).start()

    def cross(c):
        at = cut(c)
        part[at, :] += jnp.dot(feats[2, at, :], weights[2], preferred_element_type=f32)

    def finish(c):
        at = cut(c)
        forward(c).wait_recv()
        total = part[at, :] + jnp.dot(
            feats[3, at, :], weights[3], preferred_element_type=f32
        )
        of_low, of_high = total[:piece], total[piece:]
        for d in [*range(1, seqs), 0]:
            target = (seq + d) % seqs
            chosen = jnp.where(
                low == target, of_low, jnp.where(high == target, of_high, 0.0)
            ).astype(bf16)
            if d == 0:
                z_in[c // turns, 0, pl.ds((c % turns) * piece, piece), :] = chosen
            else:
                z_out[d - 1, pl.ds(c * piece, piece), :] = chosen
                z_copy(c, d).start()

    meet(0)
    cross(0)

    @pl.loop(1, chunks)
    def _(c):
        meet(c)
        finish(c - 1)
        cross(c)

    finish(chunks - 1)

    def arrive(first, last):
        @pl.loop(first, last)
        def _(c):
            for d in range(1, seqs):
                z_copy(c, d).wait_recv()

    def placed(g):
        arrived = z_in[g].reshape(seqs * group, 2 * cols)
        return jnp.dot(place[g], arrived, preferred_element_type=f32)

    arrive(0, turns)
    cache[...] = placed(0)

    @pl.loop(0, chunks)
    def _(c):
        x_copy(c).wait_send()
        forward(c).wait_send()
        for d in range(1, seqs):
            z_copy(c, d).wait_send()

    own.wait_send()
    for d in range(1, seqs):
        i_copy(d).wait_send()
    arrive(turns, chunks)
    both = (cache[...] + placed(1)).astype(bf16)
    k_out[...] = both[:, :cols]
    v_out[...] = both[:, cols:]


def store(k_in, v_in, k_out, v_out, sems):
    copies = [
        pltpu.make_async_copy(k_in, k_out, sems.at[0]),
        pltpu.make_async_copy(v_in, v_out, sems.at[1]),
    ]
    for copy in copies:
        copy.start()
    for copy in copies:
        copy.wait()


def fused(seqs, draft_features, w_key, w_value, accepted, owner_group, page_slot):
    rows, depth = draft_features.shape
    cols = w_key.shape[1]
    requests = accepted.shape[0]
    draft = rows // requests
    slots = max(2, 2 * requests // seqs) * seqs
    chunks = 8
    sent = rows // 2
    if 2 * (slots // seqs) != requests:
        return plain(draft_features, w_key, w_value, accepted, owner_group, page_slot)
    dma = pltpu.SemaphoreType.DMA
    hbm_spec = pl.BlockSpec(memory_space=pltpu.HBM)
    vmem_spec = pl.BlockSpec(memory_space=pltpu.VMEM)
    bf16 = jnp.bfloat16
    key_cache, value_cache = pl.pallas_call(
        functools.partial(kernel, (seqs, chunks, draft)),
        out_shape=(jax.ShapeDtypeStruct((slots * draft, cols), bf16),) * 2,
        in_specs=[hbm_spec] * 6,
        out_specs=(vmem_spec, vmem_spec),
        scratch_shapes=[
            pltpu.VMEM((rows, depth), bf16),
            pltpu.VMEM((4, rows, depth), bf16),
            pltpu.VMEM((4, depth, 2 * cols), bf16),
            pltpu.VMEM((rows, 2 * cols), jnp.float32),
            pltpu.VMEM((seqs - 1, sent, 2 * cols), bf16),
            pltpu.VMEM((2, seqs, sent // 2, 2 * cols), bf16),
            pltpu.VMEM((seqs - 1, 8, sent), jnp.int32),
            pltpu.VMEM((seqs, 8, sent), jnp.int32),
            pltpu.VMEM((2, slots * draft, seqs * sent // 2), bf16),
            pltpu.VMEM((slots * draft, 2 * cols), jnp.float32),
            pltpu.VMEM((1, requests), jnp.int32),
            pltpu.VMEM((1, requests), jnp.int32),
            pltpu.VMEM((1, requests), jnp.int32),
            dma, dma((4, 2)), dma((3,)),
            dma((chunks,)), dma((chunks,)), dma, dma, dma((chunks,)), dma((chunks,)),
            dma((seqs - 1, chunks)), dma((seqs - 1, chunks)),
            dma((seqs - 1,)), dma((seqs - 1,)),
        ],
        compiler_params=pltpu.CompilerParams(
            collective_id=0, has_side_effects=True, vmem_limit_bytes=48 << 20
        ),
        name="import_rows",
    )(
        *(
            pltpu.with_memory_space_constraint(x, pltpu.HBM)
            for x in (
                draft_features, w_key, w_value,
                accepted.reshape(1, requests), owner_group.reshape(1, requests),
                page_slot.reshape(1, requests),
            )
        )
    )
    key_cache, value_cache = pl.pallas_call(
        store,
        out_shape=(jax.ShapeDtypeStruct((slots * draft, cols), bf16),) * 2,
        in_specs=[vmem_spec] * 2,
        out_specs=(hbm_spec, hbm_spec),
        scratch_shapes=[dma((2,))],
        compiler_params=pltpu.CompilerParams(vmem_limit_bytes=8 << 20),
        name="store",
    )(key_cache, value_cache)
    return (
        key_cache.reshape(slots, draft, cols),
        value_cache.reshape(slots, draft, cols),
    )


def solution(mesh):
    placed = (
        P(("grp", "seq"), "head"),
        P(None, "head"),
        P(None, "head"),
        P(("grp", "seq")),
        P(("grp", "seq")),
        P(("grp", "seq")),
    )
    seqs = mesh.shape["seq"]
    local = functools.partial(fused, seqs) if mesh.shape["head"] == 4 else plain
    return jax.shard_map(
        local,
        mesh=mesh,
        in_specs=placed,
        out_specs=(P(("grp", "seq"), None, "head"), P(("grp", "seq"), None, "head")),
        check_vma=False,
    )
```

```python
import functools

import jax
import jax.numpy as jnp
from jax import lax
from jax.experimental import pallas as pl
from jax.experimental.pallas import tpu as pltpu
from jax.sharding import PartitionSpec as P

MESH = pl.DeviceIdType.MESH


def pair_slots(owner_ids, slot_cap):
    row_count = owner_ids.shape[-1]
    same_owner = owner_ids[..., :, None] == owner_ids[..., None, :]
    before = lax.broadcasted_iota(jnp.int32, (row_count, row_count), 1) < lax.broadcasted_iota(
        jnp.int32, (row_count, row_count), 0
    )
    within = jnp.sum(jnp.where(same_owner & before, 1, 0), axis=-1).astype(jnp.int32)
    return owner_ids * slot_cap + within


def one_hot(labels, columns):
    return (
        labels[:, None] == lax.broadcasted_iota(jnp.int32, (labels.shape[0], columns), 1)
    ).astype(jnp.bfloat16)


def pack_rows(payload, slot_ids, slot_total):
    select = one_hot(slot_ids, slot_total)
    packed = lax.dot_general(
        select, payload, (((0,), (0,)), ((), ())), preferred_element_type=jnp.float32
    )
    return packed.astype(jnp.bfloat16)


def placement(all_owner, all_page, owner_self, req_dev, slot_cap, seq_count):
    slot_total = slot_cap * seq_count
    slot_ids = pair_slots(all_owner.reshape(seq_count, req_dev), slot_cap).reshape(-1)
    source = lax.broadcasted_iota(jnp.int32, (seq_count, req_dev), 0).reshape(-1)
    column = source * slot_cap + slot_ids - all_owner * slot_cap
    target = jnp.where(all_owner == owner_self, all_page, -1)
    to_page = one_hot(target, slot_total)
    from_column = one_hot(column, slot_total)
    placing = lax.dot_general(
        to_page, from_column, (((0,), (0,)), ((), ())), preferred_element_type=jnp.float32
    )
    return placing.astype(jnp.bfloat16)


def plain(draft_features, w_key, w_value, accepted, owner_group, page_slot):
    req_dev = accepted.shape[0]
    draft_rows = draft_features.shape[0] // req_dev
    head_cols = w_key.shape[1]
    seq_count = lax.axis_size("seq")
    owner_self = lax.axis_index("seq")
    slot_cap = max(2, 2 * req_dev // seq_count)
    slot_total = slot_cap * seq_count
    send_slots = pair_slots(owner_group, slot_cap)
    live_rows = lax.broadcasted_iota(jnp.int32, (req_dev, draft_rows), 1) < accepted[:, None]
    all_owner, all_page = (
        lax.all_gather(owner_group, "seq", axis=0, tiled=True),
        lax.all_gather(page_slot, "seq", axis=0, tiled=True),
    )
    placing = placement(all_owner, all_page, owner_self, req_dev, slot_cap, seq_count)
    portion = lax.all_gather(draft_features, "head", axis=1, tiled=True)
    key_sum = jnp.dot(portion, w_key, preferred_element_type=jnp.float32)
    value_sum = jnp.dot(portion, w_value, preferred_element_type=jnp.float32)
    key_local = jnp.where(
        live_rows[:, :, None], key_sum.reshape(req_dev, draft_rows, head_cols), 0.0
    )
    value_local = jnp.where(
        live_rows[:, :, None], value_sum.reshape(req_dev, draft_rows, head_cols), 0.0
    )
    key_local = key_local.astype(jnp.bfloat16).reshape(req_dev, draft_rows * head_cols)
    value_local = value_local.astype(jnp.bfloat16).reshape(req_dev, draft_rows * head_cols)
    key_send = pack_rows(key_local, send_slots, slot_total)
    value_send = pack_rows(value_local, send_slots, slot_total)
    key_arrived, value_arrived = (
        lax.all_to_all(key_send, "seq", split_axis=0, concat_axis=0, tiled=True),
        lax.all_to_all(value_send, "seq", split_axis=0, concat_axis=0, tiled=True),
    )
    key_cache = jnp.dot(placing, key_arrived, preferred_element_type=jnp.float32).astype(
        jnp.bfloat16
    )
    value_cache = jnp.dot(placing, value_arrived, preferred_element_type=jnp.float32).astype(
        jnp.bfloat16
    )
    return (
        key_cache.reshape(slot_total, draft_rows, head_cols),
        value_cache.reshape(slot_total, draft_rows, head_cols),
    )


def kernel(
    dims, f_hbm, wk_hbm, wv_hbm, acc_hbm, own_hbm, page_hbm, k_out, v_out,
    raw, feats, weights, part, z_out, z_in, key_out, key_in, place, cache,
    acc_ref, own_ref, page_ref,
    load_sem, w_sem, id_sem, x_send, x_recv, d_send, d_recv, f_send, f_recv,
    z_send, z_recv, i_send, i_recv,
):
    seqs, chunks, draft = dims
    rows, depth = f_hbm.shape
    cols = wk_hbm.shape[1]
    step = rows // chunks
    requests = rows // draft
    cap = requests // 2
    share = cap // chunks
    piece = share * draft
    group = cap * draft // 2
    turns = chunks // 2
    slot_rows = k_out.shape[0]
    bf16, f32, i32 = jnp.bfloat16, jnp.float32, jnp.int32
    head = lax.axis_index("head")
    seq = lax.axis_index("seq")
    partner = head + 1 - 2 * (head % 2)
    across = (head + 2) % 4
    blocks = (head, partner, across, (partner + 2) % 4)

    id_loads = [
        pltpu.make_async_copy(src, dst, id_sem.at[n])
        for n, (src, dst) in enumerate(
            ((own_hbm, own_ref), (acc_hbm, acc_ref), (page_hbm, page_ref))
        )
    ]
    for id_load in id_loads:
        id_load.start()
    load = pltpu.make_async_copy(f_hbm, raw, load_sem)
    load.start()
    w_loads = []
    for k in range(4):
        at = pl.ds(pl.multiple_of(blocks[k] * depth, depth), depth)
        for n, w in enumerate((wk_hbm, wv_hbm)):
            w_loads.append(
                pltpu.make_async_copy(
                    w.at[at, :], weights.at[k, :, pl.ds(n * cols, cols)], w_sem.at[k, n]
                )
            )

    barrier = pltpu.get_barrier_semaphore()
    peers = [{"head": partner}, {"head": across}]
    peers += [{"seq": (seq + d) % seqs} for d in range(1, seqs)]
    for peer in peers:
        pl.semaphore_signal(barrier, inc=1, device_id=peer, device_id_type=MESH)
    for w_load in w_loads:
        w_load.start()

    def iota(shape, dim):
        return lax.broadcasted_iota(i32, shape, dim)

    def exact(values, table, dims=(((1,), (0,)), ((), ()))):
        return lax.dot_general(
            values.astype(bf16), table.astype(bf16), dims, preferred_element_type=f32
        )

    for id_load in id_loads:
        id_load.wait()
    owner = own_ref[...]
    low = jnp.min(owner, axis=1, keepdims=True)
    high = jnp.max(owner, axis=1, keepdims=True)
    mine = (iota((8, requests), 0) == owner).astype(f32)
    earlier = (iota((requests, requests), 0) < iota((requests, requests), 1)).astype(f32)
    rank = jnp.sum(mine * exact(mine, earlier), axis=0, keepdims=True).astype(i32)
    spot = (rank // share) * (2 * share) + rank % share + jnp.where(owner > low, share, 0)
    spread = (iota((requests, rows), 1) // draft == iota((requests, rows), 0)).astype(f32)
    wide = exact(jnp.broadcast_to(spot.astype(f32), (8, requests)), spread)
    goal = wide.astype(i32)[0:1, :] * draft + iota((1, rows), 1) % draft
    order = (iota((rows, rows), 0) == goal).astype(bf16)

    load.wait()

    def remote(src, dst, send_sem, recv_sem, peer):
        return pltpu.make_async_remote_copy(
            src_ref=src, dst_ref=dst, send_sem=send_sem, recv_sem=recv_sem,
            device_id=peer, device_id_type=MESH,
        )

    def cut(c):
        return pl.ds(c * step, step)

    def x_copy(c):
        return remote(
            feats.at[0, cut(c), :], feats.at[2, cut(c), :], x_send.at[c], x_recv.at[c],
            {"head": across},
        )

    def forward(c):
        return remote(
            feats.at[2, cut(c), :], feats.at[3, cut(c), :], f_send.at[c], f_recv.at[c],
            {"head": partner},
        )

    def z_copy(c, d):
        at = pl.ds(c * piece, piece)
        there = pl.ds((c % turns) * piece, piece)
        return remote(
            z_out.at[d - 1, at, :], z_in.at[c // turns, d, there, :],
            z_send.at[d - 1, c], z_recv.at[d - 1, c], {"seq": (seq + d) % seqs},
        )

    def i_copy(d):
        return remote(
            key_out.at[d - 1], key_in.at[d], i_send.at[d - 1], i_recv.at[d - 1],
            {"seq": (seq + d) % seqs},
        )

    early = 2
    for first, last in ((0, early), (early, chunks)):
        some = slice(first * step, last * step)
        feats[0, some, :] = jnp.dot(
            order[some], raw[...], preferred_element_type=f32
        ).astype(bf16)
        if first == 0:
            pl.semaphore_wait(barrier, len(peers))
        for c in range(first, last):
            x_copy(c).start()
    own = remote(feats.at[0], feats.at[1], d_send, d_recv, {"head": partner})
    own.start()

    page = jnp.broadcast_to(page_ref[...].astype(f32), (8, requests))
    live = jnp.broadcast_to(acc_ref[...].astype(f32), (8, requests))
    within = iota((8, cap * draft), 1) % draft
    last_dims = (((1,), (1,)), ((), ()))
    for d in range(seqs):
        taken = (
            (owner == (seq + d) % seqs) & (rank == iota((cap * draft, requests), 0) // draft)
        ).astype(f32)
        key = jnp.where(
            within < exact(live, taken, last_dims).astype(i32),
            exact(page, taken, last_dims).astype(i32) * draft + within,
            -1,
        )
        if d == 0:
            key_in[0] = key
        else:
            key_out[d - 1] = key
            i_copy(d).start()

    w_loads[0].wait()
    w_loads[1].wait()
    part[...] = jnp.dot(feats[0], weights[0], preferred_element_type=f32)
    own.wait_recv()
    w_loads[2].wait()
    w_loads[3].wait()
    part[...] += jnp.dot(feats[1], weights[1], preferred_element_type=f32)

    for d in range(seqs):
        if d > 0:
            i_copy(d).wait_recv()
        placing = (iota((slot_rows, cap * draft), 0) == key_in[d][0:1, :]).astype(bf16)
        for g in range(2):
            place[g, :, d * group : (d + 1) * group] = placing[:, g * group : (g + 1) * group]
    for w_load in w_loads[4:]:
        w_load.wait()

    def meet(c):
        x_copy(c).wait_recv()
        forward(c).start()

    def cross(c):
        at = cut(c)
        part[at, :] += jnp.dot(feats[2, at, :], weights[2], preferred_element_type=f32)

    def finish(c):
        at = cut(c)
        forward(c).wait_recv()
        total = part[at, :] + jnp.dot(
            feats[3, at, :], weights[3], preferred_element_type=f32
        )
        of_low, of_high = total[:piece], total[piece:]
        upper = (2 * seq) // seqs
        far = [upper * k + (1 - upper) * (seqs - k) for k in range(1, seqs)]
        for d in [*far, 0]:
            target = (seq + d) % seqs
            chosen = jnp.where(
                low == target, of_low, jnp.where(high == target, of_high, 0.0)
            ).astype(bf16)
            if isinstance(d, int):
                z_in[c // turns, 0, pl.ds((c % turns) * piece, piece), :] = chosen
            else:
                z_out[d - 1, pl.ds(c * piece, piece), :] = chosen
                z_copy(c, d).start()

    meet(0)
    cross(0)

    @pl.loop(1, chunks)
    def _(c):
        meet(c)
        finish(c - 1)
        cross(c)

    finish(chunks - 1)

    def arrive(first, last):
        @pl.loop(first, last)
        def _(c):
            for d in range(1, seqs):
                z_copy(c, d).wait_recv()

    def placed(g):
        arrived = z_in[g].reshape(seqs * group, 2 * cols)
        return jnp.dot(place[g], arrived, preferred_element_type=f32)

    arrive(0, turns)
    cache[...] = placed(0)

    @pl.loop(0, chunks)
    def _(c):
        x_copy(c).wait_send()
        forward(c).wait_send()
        for d in range(1, seqs):
            z_copy(c, d).wait_send()

    own.wait_send()
    for d in range(1, seqs):
        i_copy(d).wait_send()
    arrive(turns, chunks)
    both = (cache[...] + placed(1)).astype(bf16)
    k_out[...] = both[:, :cols]
    v_out[...] = both[:, cols:]


def store(k_in, v_in, k_out, v_out, sems):
    copies = [
        pltpu.make_async_copy(k_in, k_out, sems.at[0]),
        pltpu.make_async_copy(v_in, v_out, sems.at[1]),
    ]
    for copy in copies:
        copy.start()
    for copy in copies:
        copy.wait()


def fused(seqs, draft_features, w_key, w_value, accepted, owner_group, page_slot):
    rows, depth = draft_features.shape
    cols = w_key.shape[1]
    requests = accepted.shape[0]
    draft = rows // requests
    slots = max(2, 2 * requests // seqs) * seqs
    chunks = 8
    sent = rows // 2
    if 2 * (slots // seqs) != requests:
        return plain(draft_features, w_key, w_value, accepted, owner_group, page_slot)
    dma = pltpu.SemaphoreType.DMA
    hbm_spec = pl.BlockSpec(memory_space=pltpu.HBM)
    vmem_spec = pl.BlockSpec(memory_space=pltpu.VMEM)
    bf16 = jnp.bfloat16
    key_cache, value_cache = pl.pallas_call(
        functools.partial(kernel, (seqs, chunks, draft)),
        out_shape=(jax.ShapeDtypeStruct((slots * draft, cols), bf16),) * 2,
        in_specs=[hbm_spec] * 6,
        out_specs=(vmem_spec, vmem_spec),
        scratch_shapes=[
            pltpu.VMEM((rows, depth), bf16),
            pltpu.VMEM((4, rows, depth), bf16),
            pltpu.VMEM((4, depth, 2 * cols), bf16),
            pltpu.VMEM((rows, 2 * cols), jnp.float32),
            pltpu.VMEM((seqs - 1, sent, 2 * cols), bf16),
            pltpu.VMEM((2, seqs, sent // 2, 2 * cols), bf16),
            pltpu.VMEM((seqs - 1, 8, sent), jnp.int32),
            pltpu.VMEM((seqs, 8, sent), jnp.int32),
            pltpu.VMEM((2, slots * draft, seqs * sent // 2), bf16),
            pltpu.VMEM((slots * draft, 2 * cols), jnp.float32),
            pltpu.VMEM((1, requests), jnp.int32),
            pltpu.VMEM((1, requests), jnp.int32),
            pltpu.VMEM((1, requests), jnp.int32),
            dma, dma((4, 2)), dma((3,)),
            dma((chunks,)), dma((chunks,)), dma, dma, dma((chunks,)), dma((chunks,)),
            dma((seqs - 1, chunks)), dma((seqs - 1, chunks)),
            dma((seqs - 1,)), dma((seqs - 1,)),
        ],
        compiler_params=pltpu.CompilerParams(
            collective_id=0, has_side_effects=True, vmem_limit_bytes=48 << 20
        ),
        name="import_rows",
    )(
        *(
            pltpu.with_memory_space_constraint(x, pltpu.HBM)
            for x in (
                draft_features, w_key, w_value,
                accepted.reshape(1, requests), owner_group.reshape(1, requests),
                page_slot.reshape(1, requests),
            )
        )
    )
    key_cache, value_cache = pl.pallas_call(
        store,
        out_shape=(jax.ShapeDtypeStruct((slots * draft, cols), bf16),) * 2,
        in_specs=[vmem_spec] * 2,
        out_specs=(hbm_spec, hbm_spec),
        scratch_shapes=[dma((2,))],
        compiler_params=pltpu.CompilerParams(vmem_limit_bytes=8 << 20),
        name="store",
    )(key_cache, value_cache)
    return (
        key_cache.reshape(slots, draft, cols),
        value_cache.reshape(slots, draft, cols),
    )


def solution(mesh):
    placed = (
        P(("grp", "seq"), "head"),
        P(None, "head"),
        P(None, "head"),
        P(("grp", "seq")),
        P(("grp", "seq")),
        P(("grp", "seq")),
    )
    seqs = mesh.shape["seq"]
    local = functools.partial(fused, seqs) if mesh.shape["head"] == 4 else plain
    return jax.shard_map(
        local,
        mesh=mesh,
        in_specs=placed,
        out_specs=(P(("grp", "seq"), None, "head"), P(("grp", "seq"), None, "head")),
        check_vma=False,
    )
```
